512 devices in a mesh: dp: 32 (over x, y), mx: 4 (over z_hi, core), my: 4 (over z_lo).
Axes of the slice: x: 4, y: 8, z: 8 (z_hi: 2, z_lo: 4; z = z_hi * 4 + z_lo), core: 2. Of those that a mesh axis runs over, the one named last changes fastest.
Arguments:
- mentor_final_states: bfloat16 [2048, 4608], P('dp'), may hold values from -12 to 12
- mentor_output_matrix: bfloat16 [4608, 4096], P(None, ('mx', 'my')), may hold values from -0.09375 to 0.09375
- learner_final_states: bfloat16 [2048, 3584], P('dp', 'mx'), may hold values from -12 to 12
- learner_output_matrix: bfloat16 [3584, 4096], P('mx', 'my'), may hold values from -0.09375 to 0.09375
- loss_mask: int32 [2048], P('dp'), may hold values 0 or 1
Outputs:
- mismatch_per_piece: float32 [2048], P('dp')
- mean_loss: float32 [], replicated
- student_grad: float32 [2048, 4096], P('dp', 'my')
The draws below stay inside these ranges and needn't reach their ends.
All inputs are finite; a program needn't handle non-finite values.
Results may differ from the reference program's by a relative error of at most 0.0003.
Values sent between devices are 32-bit elements.
A program may use at most 64 MiB of HBM per device.

```python
import jax
import jax.numpy as jnp

D_T = 4608
D_S = 3584
WORD_LEXICON = 4096
WINDOW_PIECES = 2048


def with_ends(array, key, least, high):
    dims = array.shape
    place = [jax.random.randint(jax.random.fold_in(key, axis), (), 0, dims[axis]) for axis in range(len(dims))]
    array = array.at[tuple(place)].set(least)
    longest = dims.index(max(dims))
    place[longest] = (place[longest] + 1) % dims[longest]
    return array.at[tuple(place)].set(high)


def steps_of(own_key, shape, pieces, smallest, largest):
    def one(dim, shards_of):
        draws = jax.random.uniform(jax.random.fold_in(jax.random.fold_in(own_key, 6), dim), (shards_of,), jnp.float32, smallest / len(pieces), largest / len(pieces))
        return jnp.repeat(jnp.exp(draws), shape[dim] // shards_of).reshape((-1,) + (1,) * (len(shape) - dim - 1))

    level = one(*pieces[0])
    for cut in pieces[1:]:
        level = level * one(*cut)
    return level


def bell_draw(own_key, extent, spread, limit, cuts=(), kind=jnp.bfloat16):
    result = spread * jax.random.normal(own_key, extent, jnp.float32)
    if cuts:
        result = result * steps_of(own_key, extent, cuts, -0.22, 0.18)
    return jnp.clip(result, -limit, limit).astype(kind)


def setup_inputs(seed: int = 0) -> dict:
    arg_keys = jax.random.split(jax.random.key(seed), 6)
    mentor_final_states = bell_draw(arg_keys[0], (WINDOW_PIECES, D_T), 2.0, 12.0, ((0, 32),))
    mentor_output_matrix = bell_draw(arg_keys[1], (D_T, WORD_LEXICON), D_T ** -0.5, 0.09375, ((1, 16),))
    learner_final_states = bell_draw(arg_keys[2], (WINDOW_PIECES, D_S), 2.0, 12.0, ((0, 32), (1, 4)))
    learner_output_matrix = bell_draw(arg_keys[3], (D_S, WORD_LEXICON), D_S ** -0.5, 0.09375, ((0, 4), (1, 4)))
    loss_mask = with_ends((jax.random.randint(arg_keys[4], (WINDOW_PIECES,), 0, 4) < 3).astype(jnp.int32), jax.random.fold_in(arg_keys[4], 1), 0, 1)
    return {"mentor_final_states": mentor_final_states, "mentor_output_matrix": mentor_output_matrix, "learner_final_states": learner_final_states, "learner_output_matrix": learner_output_matrix, "loss_mask": loss_mask}


SOFTENING_HEAT = 2.0


def log_softmax_rows(values):
    row_max = jnp.max(values, axis=1, keepdims=True)
    row_sum = jnp.sum(jnp.exp(values - row_max), axis=1, keepdims=True)
    return values - (row_max + jnp.log(row_sum))


def reference(mentor_final_states, mentor_output_matrix, learner_final_states, learner_output_matrix, loss_mask):
    mentor_softened_scores = jnp.dot(mentor_final_states, mentor_output_matrix, preferred_element_type=jnp.float32) / SOFTENING_HEAT
    learner_softened_scores = jnp.dot(learner_final_states, learner_output_matrix, preferred_element_type=jnp.float32) / SOFTENING_HEAT
    mentor_logarithmic_odds = log_softmax_rows(mentor_softened_scores)
    learner_logarithmic_odds = log_softmax_rows(learner_softened_scores)
    mentor_likelihoods = jnp.exp(mentor_logarithmic_odds)
    mismatch_per_piece = SOFTENING_HEAT * SOFTENING_HEAT * jnp.sum(mentor_likelihoods * (mentor_logarithmic_odds - learner_logarithmic_odds), axis=1)
    piece_importance = loss_mask.astype(jnp.float32)
    usable_count = jnp.sum(piece_importance)
    mean_loss = jnp.sum(piece_importance * mismatch_per_piece) / usable_count
    multiplier = piece_importance * (SOFTENING_HEAT * WORD_LEXICON * WINDOW_PIECES) / usable_count
    student_grad = (jnp.exp(learner_logarithmic_odds) - mentor_likelihoods) * multiplier[:, None]
    return mismatch_per_piece, mean_loss, student_grad
```

```python
import functools

import jax
import jax.numpy as jnp
from jax import lax
from jax.experimental import pallas as pl
from jax.experimental.pallas import tpu as pltpu
from jax.sharding import Mesh
from jax.sharding import PartitionSpec as P

DP = ("dp_0", "dp_1")
MESH = pl.DeviceIdType.MESH
HEAT = 2.0
CHUNKS = 6


def kernel(
    sizes,
    scale,
    xt_hbm,
    wt_hbm,
    xs_hbm,
    ws_hbm,
    mask_ref,
    grad_ref,
    mis_ref,
    loss_ref,
    xt,
    wt,
    xs,
    ws,
    psend,
    precv,
    csum,
    recv1,
    gblk,
    stats,
    cnt_x,
    cnt_y,
    los_x,
    los_y,
    ld_sem,
    d_send,
    d_recv,
    p1_send,
    p1_recv,
    st_send,
    st_recv,
    g_send,
    g_recv,
    f_send,
    f_recv,
    x_send,
    x_recv,
    y_send,
    y_recv,
):
    nx, ny, nk, ni = sizes
    ix = lax.axis_index("dp_0")
    iy = lax.axis_index("dp_1")
    k = lax.axis_index("mx")
    i = lax.axis_index("my")
    c = lax.rem(k, 2)
    zh = lax.div(k, 2)
    partner = k + 1 - 2 * c
    tokens, width = csum.shape[1], csum.shape[2]
    deep = wt.shape[0] // CHUNKS

    barrier = pltpu.get_barrier_semaphore()
    peers = []
    for dk in range(nk):
        for di in range(ni):
            if dk or di:
                peers.append({"mx": lax.rem(k + dk, nk), "my": lax.rem(i + di, ni)})
    xpeers = [{"dp_0": lax.rem(ix + d, nx)} for d in range(1, nx)]
    ypeers = [{"dp_1": lax.rem(iy + d, ny)} for d in range(1, ny)]
    for peer in peers + xpeers + ypeers:
        pl.semaphore_signal(barrier, inc=1, device_id=peer, device_id_type=MESH)

    loads = [pltpu.make_async_copy(xs_hbm, xs, ld_sem.at[0])]
    order = [c, 2 + c, 1 - c, 3 - c]
    for n, j in enumerate(order):
        cols = pl.ds(pl.multiple_of(j * width, width), width)
        loads.append(pltpu.make_async_copy(ws_hbm.at[:, cols], ws.at[n], ld_sem.at[1 + n]))
    loads.append(pltpu.make_async_copy(xt_hbm, xt, ld_sem.at[5]))
    for n in range(CHUNKS):
        rows = pl.ds(n * deep, deep)
        loads.append(pltpu.make_async_copy(wt_hbm.at[rows], wt.at[rows], ld_sem.at[6 + n]))
    for copy in loads:
        copy.start()

    def student(n):
        loads[1 + n].wait()
        return jnp.dot(xs[...], ws[n], preferred_element_type=jnp.float32)

    def remote(src, dst, send, recv, peer):
        return pltpu.make_async_remote_copy(
            src_ref=src, dst_ref=dst, send_sem=send, recv_sem=recv, device_id=peer, device_id_type=MESH
        )

    mask = mask_ref[...].astype(jnp.float32)
    cnt_x[ix] = jnp.full((1, 128), jnp.sum(mask), jnp.float32)

    loads[0].wait()
    swaps = []
    for n in range(2):
        psend[n] = student(n)
        if n == 0:
            pl.semaphore_wait(barrier, len(peers + xpeers + ypeers))
        copy = remote(psend.at[n], precv.at[n], d_send.at[n], d_recv.at[n], {"mx": partner})
        copy.start()
        swaps.append(copy)

    def spread(buf, me, stage, send, recv, peer_list):
        copies = []
        for d, peer in enumerate(peer_list):
            copies.append(remote(buf.at[me], buf.at[me], send.at[stage, d], recv.at[stage, d], peer))
        for copy in copies:
            copy.start()
        return copies

    first = []
    for n in range(2):
        own = student(2 + n)
        swaps[n].wait_recv()
        csum[n] = own + precv[n]
        j = 2 * n + 1 - c
        copy = remote(csum.at[n], recv1.at[zh], p1_send.at[n], p1_recv.at[zh], {"mx": i, "my": j})
        copy.start()
        first.append(copy)

    cx = spread(cnt_x, ix, 0, x_send, x_recv, xpeers)

    loads[5].wait()
    acc = jnp.zeros((tokens, width), jnp.float32)
    for n in range(CHUNKS):
        loads[6 + n].wait()
        rows = pl.ds(n * deep, deep)
        acc = acc + jnp.dot(xt[:, rows], wt[rows, :], preferred_element_type=jnp.float32)
    t = acc * (1.0 / HEAT)
    t_max = jnp.max(t, axis=1, keepdims=True)
    t_exp = jnp.exp(t - t_max)
    t_sum = jnp.sum(t_exp, axis=1, keepdims=True)
    t_lse = t_max + jnp.log(t_sum)

    for copy in cx:
        copy.wait_recv()
    cnt_y[iy] = jnp.sum(cnt_x[...], axis=0)
    cy = spread(cnt_y, iy, 0, y_send, y_recv, ypeers)

    for h in range(2):
        pltpu.make_async_copy(recv1.at[h], recv1.at[h], p1_recv.at[h]).wait()
    s = (recv1[0] + recv1[1]) * (1.0 / HEAT)
    s_max = jnp.max(s, axis=1, keepdims=True)
    s_sum = jnp.sum(jnp.exp(s - s_max), axis=1, keepdims=True)
    s_lse = s_max + jnp.log(s_sum)
    gap = jnp.sum(t_exp * (t - s), axis=1, keepdims=True) / t_sum

    row_id = lax.broadcasted_iota(jnp.int32, (tokens, 2 * tokens), 0)
    lane_id = lax.broadcasted_iota(jnp.int32, (tokens, 2 * tokens), 1)
    low = lane_id < tokens
    eye2 = (lane_id == row_id) | (lane_id == row_id + tokens)
    me = k * ni + i
    both = jnp.where(eye2, jnp.where(low, t_lse, s_lse), 0.0)
    gaps = jnp.where(eye2, jnp.broadcast_to(gap, both.shape), 0.0)
    stats[me, 0:1] = jnp.sum(both, axis=0, keepdims=True)
    stats[me, 1:2] = jnp.sum(gaps, axis=0, keepdims=True)
    sts = []
    for d, peer in enumerate(peers):
        sts.append(remote(stats.at[me], stats.at[me], st_send.at[d], st_recv.at[d], peer))
    for copy in sts:
        copy.start()
    for copy in cy:
        copy.wait_recv()
    count = jnp.sum(cnt_y[...], axis=0)
    for copy in sts:
        copy.wait_recv()

    lse = [stats[g, 0:1] for g in range(nk * ni)]
    top = functools.reduce(jnp.maximum, lse)
    weights = [jnp.exp(v - top) for v in lse]
    total = functools.reduce(jnp.add, weights)
    z = top + jnp.log(total)
    num = functools.reduce(jnp.add, [w * stats[g, 1:2] for g, w in enumerate(weights)])
    zt = z[:, :tokens]
    zs = z[:, tokens:]
    kl = (HEAT * HEAT) * (num[:, :tokens] / total[:, :tokens] - zt + zs)
    mis_ref[...] = kl
    los_x[ix] = jnp.full((1, 128), jnp.sum(mask * kl), jnp.float32)
    lx = spread(los_x, ix, 1, x_send, x_recv, xpeers)

    eye = (
        lax.broadcasted_iota(jnp.int32, (tokens, tokens), 0)
        == lax.broadcasted_iota(jnp.int32, (tokens, tokens), 1)
    )

    def column(row):
        return jnp.sum(jnp.where(eye, row, 0.0), axis=1, keepdims=True)

    factor = column(mask * scale / count[:, :tokens])
    gblk[...] = (jnp.exp(s - column(zs)) - jnp.exp(t - column(zt))) * factor
    outs = []
    mycols = pl.ds(pl.multiple_of(i * width, width), width)
    r = 1 - lax.rem(i, 2)
    for h in range(2):
        outs.append(
            remote(gblk, grad_ref.at[:, mycols], g_send.at[h], g_recv.at[lax.div(i, 2)], {"mx": 2 * h + r, "my": k})
        )
    for copy in outs:
        copy.start()

    for copy in lx:
        copy.wait_recv()
    los_y[iy] = jnp.sum(los_x[...], axis=0)
    ly = spread(los_y, iy, 1, y_send, y_recv, ypeers)

    forwards = []
    for n in range(2):
        j = 2 * n + 1 - c
        cols = pl.ds(pl.multiple_of(j * width, width), width)
        block = grad_ref.at[:, cols]
        pltpu.make_async_copy(block, block, g_recv.at[n]).wait()
        copy = remote(block, block, f_send.at[n], f_recv.at[n], {"mx": partner})
        copy.start()
        forwards.append(copy)

    for copy in ly:
        copy.wait_recv()
    loss_ref[...] = jnp.sum(los_y[...], axis=0) / count
    for copy in forwards:
        copy.wait_recv()
    for copy in swaps + first + cx + cy + sts + lx + outs + ly + forwards:
        copy.wait_send()


def local(xt, wt, xs, ws, mask):
    nx, ny, nk, ni = (lax.axis_size(a) for a in ("dp_0", "dp_1", "mx", "my"))
    tokens, depth_t = xt.shape
    width = wt.shape[1]
    depth_s, span = ws.shape
    scale = HEAT * width * nk * ni * tokens * nx * ny
    f32 = jnp.float32
    dma = pltpu.SemaphoreType.DMA
    vmem = pl.BlockSpec(memory_space=pltpu.VMEM)
    hbm = pl.BlockSpec(memory_space=pl.ANY)
    grad, mis, loss = pl.pallas_call(
        functools.partial(kernel, (nx, ny, nk, ni), scale),
        out_shape=(
            jax.ShapeDtypeStruct((tokens, span), f32),
            jax.ShapeDtypeStruct((1, tokens), f32),
            jax.ShapeDtypeStruct((1, 128), f32),
        ),
        in_specs=[hbm, hbm, hbm, hbm, vmem],
        out_specs=(vmem, vmem, vmem),
        scratch_shapes=[
            pltpu.VMEM((tokens, depth_t), jnp.bfloat16),
            pltpu.VMEM((depth_t, width), jnp.bfloat16),
            pltpu.VMEM((tokens, depth_s), jnp.bfloat16),
            pltpu.VMEM((4, depth_s, width), jnp.bfloat16),
            pltpu.VMEM((2, tokens, width), f32),
            pltpu.VMEM((2, tokens, width), f32),
            pltpu.VMEM((2, tokens, width), f32),
            pltpu.VMEM((2, tokens, width), f32),
            pltpu.VMEM((tokens, width), f32),
            pltpu.VMEM((nk * ni, 2, 128), f32),
            pltpu.VMEM((nx, 1, 128), f32),
            pltpu.VMEM((ny, 1, 128), f32),
            pltpu.VMEM((nx, 1, 128), f32),
            pltpu.VMEM((ny, 1, 128), f32),
            dma((6 + CHUNKS,)),
            dma((2,)),
            dma((2,)),
            dma((2,)),
            dma((2,)),
            dma((nk * ni,)),
            dma((nk * ni,)),
            dma((2,)),
            dma((2,)),
            dma((2,)),
            dma((2,)),
            dma((2, nx)),
            dma((2, nx)),
            dma((2, ny)),
            dma((2, ny)),
        ],
        compiler_params=pltpu.CompilerParams(collective_id=0, has_side_effects=True),
    )(xt, wt, xs, ws, mask.reshape(1, tokens))
    return mis.reshape(tokens), loss[0, 0], grad


def solution(mesh):
    split = Mesh(
        mesh.devices.reshape(4, 8, mesh.shape["mx"], mesh.shape["my"]), ("dp_0", "dp_1", "mx", "my")
    )
    in_specs = (P(DP, None), P(None, ("mx", "my")), P(DP, "mx"), P("mx", "my"), P(DP))
    out_specs = (P(DP), P(), P(DP, "my"))
    return jax.shard_map(local, mesh=split, in_specs=in_specs, out_specs=out_specs, check_vma=False)
```

```python
import functools

import jax
import jax.numpy as jnp
from jax import lax
from jax.experimental import pallas as pl
from jax.experimental.pallas import tpu as pltpu
from jax.sharding import Mesh
from jax.sharding import PartitionSpec as P

DP = ("dp_0", "dp_1")
MESH = pl.DeviceIdType.MESH
HEAT = 2.0
CHUNKS = 6


def kernel(
    sizes,
    scale,
    xt_hbm,
    wt_hbm,
    xs_hbm,
    ws_hbm,
    mask_hbm,
    grad_ref,
    mis_ref,
    loss_ref,
    xt,
    wt,
    xs,
    ws,
    mask_ref,
    psend,
    precv,
    csum,
    recv1,
    gblk,
    stats,
    cnt_x,
    cnt_y,
    los_x,
    los_y,
    ld_sem,
    d_send,
    d_recv,
    p1_send,
    p1_recv,
    st_send,
    st_recv,
    g_send,
    g_recv,
    f_send,
    f_recv,
    x_send,
    x_recv,
    y_send,
    y_recv,
):
    nx, ny, nk, ni = sizes
    ix = lax.axis_index("dp_0")
    iy = lax.axis_index("dp_1")
    k = lax.axis_index("mx")
    i = lax.axis_index("my")
    c = lax.rem(k, 2)
    zh = lax.div(k, 2)
    partner = k + 1 - 2 * c
    tokens, width = csum.shape[1], csum.shape[2]
    deep = wt.shape[0] // CHUNKS

    barrier = pltpu.get_barrier_semaphore()
    peers = []
    for dk in range(nk):
        for di in range(ni):
            if dk or di:
                peers.append({"mx": lax.rem(k + dk, nk), "my": lax.rem(i + di, ni)})
    xpeers = [{"dp_0": lax.rem(ix + d, nx)} for d in range(1, nx)]
    ypeers = [{"dp_1": lax.rem(iy + d, ny)} for d in range(1, ny)]
    for peer in peers + xpeers + ypeers:
        pl.semaphore_signal(barrier, inc=1, device_id=peer, device_id_type=MESH)

    loads = [pltpu.make_async_copy(xs_hbm, xs, ld_sem.at[0])]
    order = [c, 2 + c, 1 - c, 3 - c]
    for n, j in enumerate(order):
        cols = pl.ds(pl.multiple_of(j * width, width), width)
        loads.append(pltpu.make_async_copy(ws_hbm.at[:, cols], ws.at[n], ld_sem.at[1 + n]))
    loads.append(pltpu.make_async_copy(xt_hbm, xt, ld_sem.at[5]))
    for n in range(CHUNKS):
        rows = pl.ds(n * deep, deep)
        loads.append(pltpu.make_async_copy(wt_hbm.at[rows], wt.at[rows], ld_sem.at[6 + n]))
    loads.append(pltpu.make_async_copy(mask_hbm, mask_ref, ld_sem.at[6 + CHUNKS]))
    for copy in loads:
        copy.start()

    def student(n):
        loads[1 + n].wait()
        return jnp.dot(xs[...], ws[n], preferred_element_type=jnp.float32)

    def remote(src, dst, send, recv, peer):
        return pltpu.make_async_remote_copy(
            src_ref=src, dst_ref=dst, send_sem=send, recv_sem=recv, device_id=peer, device_id_type=MESH
        )

    loads[0].wait()
    swaps = []
    for n in range(2):
        psend[n] = student(n)
        if n == 0:
            pl.semaphore_wait(barrier, len(peers + xpeers + ypeers))
        copy = remote(psend.at[n], precv.at[n], d_send.at[n], d_recv.at[n], {"mx": partner})
        copy.start()
        swaps.append(copy)

    def spread(buf, me, stage, send, recv, peer_list):
        copies = []
        for d, peer in enumerate(peer_list):
            copies.append(remote(buf.at[me], buf.at[me], send.at[stage, d], recv.at[stage, d], peer))
        for copy in copies:
            copy.start()
        return copies

    first = []
    for n in range(2):
        own = student(2 + n)
        swaps[n].wait_recv()
        csum[n] = own + precv[n]
        j = 2 * n + 1 - c
        copy = remote(csum.at[n], recv1.at[zh], p1_send.at[n], p1_recv.at[zh], {"mx": i, "my": j})
        copy.start()
        first.append(copy)

    loads[-1].wait()
    mask = mask_ref[...].astype(jnp.float32)
    cnt_x[ix] = jnp.full((1, 128), jnp.sum(mask), jnp.float32)
    cx = spread(cnt_x, ix, 0, x_send, x_recv, xpeers)

    loads[5].wait()
    acc = jnp.zeros((tokens, width), jnp.float32)
    for n in range(CHUNKS):
        loads[6 + n].wait()
        rows = pl.ds(n * deep, deep)
        acc = acc + jnp.dot(xt[:, rows], wt[rows, :], preferred_element_type=jnp.float32)
    t = acc * (1.0 / HEAT)
    t_max = jnp.max(t, axis=1, keepdims=True)
    t_exp = jnp.exp(t - t_max)
    t_sum = jnp.sum(t_exp, axis=1, keepdims=True)
    t_lse = t_max + jnp.log(t_sum)

    for copy in cx:
        copy.wait_recv()
    cnt_y[iy] = jnp.sum(cnt_x[...], axis=0)
    cy = spread(cnt_y, iy, 0, y_send, y_recv, ypeers)

    for h in range(2):
        pltpu.make_async_copy(recv1.at[h], recv1.at[h], p1_recv.at[h]).wait()
    s = (recv1[0] + recv1[1]) * (1.0 / HEAT)
    s_max = jnp.max(s, axis=1, keepdims=True)
    s_sum = jnp.sum(jnp.exp(s - s_max), axis=1, keepdims=True)
    s_lse = s_max + jnp.log(s_sum)
    gap = jnp.sum(t_exp * (t - s), axis=1, keepdims=True) / t_sum

    row_id = lax.broadcasted_iota(jnp.int32, (tokens, 2 * tokens), 0)
    lane_id = lax.broadcasted_iota(jnp.int32, (tokens, 2 * tokens), 1)
    low = lane_id < tokens
    eye2 = (lane_id == row_id) | (lane_id == row_id + tokens)
    me = k * ni + i
    both = jnp.where(eye2, jnp.where(low, t_lse, s_lse), 0.0)
    gaps = jnp.where(eye2, jnp.broadcast_to(gap, both.shape), 0.0)
    stats[me, 0:1] = jnp.sum(both, axis=0, keepdims=True)
    stats[me, 1:2] = jnp.sum(gaps, axis=0, keepdims=True)
    sts = []
    for d, peer in enumerate(peers):
        sts.append(remote(stats.at[me], stats.at[me], st_send.at[d], st_recv.at[d], peer))
    for copy in sts:
        copy.start()
    for copy in cy:
        copy.wait_recv()
    count = jnp.sum(cnt_y[...], axis=0)
    for copy in sts:
        copy.wait_recv()

    lse = [stats[g, 0:1] for g in range(nk * ni)]
    top = functools.reduce(jnp.maximum, lse)
    weights = [jnp.exp(v - top) for v in lse]
    total = functools.reduce(jnp.add, weights)
    z = top + jnp.log(total)
    num = functools.reduce(jnp.add, [w * stats[g, 1:2] for g, w in enumerate(weights)])
    zt = z[:, :tokens]
    zs = z[:, tokens:]
    kl = (HEAT * HEAT) * (num[:, :tokens] / total[:, :tokens] - zt + zs)
    mis_ref[...] = kl
    los_x[ix] = jnp.full((1, 128), jnp.sum(mask * kl), jnp.float32)
    lx = spread(los_x, ix, 1, x_send, x_recv, xpeers)

    eye = (
        lax.broadcasted_iota(jnp.int32, (tokens, tokens), 0)
        == lax.broadcasted_iota(jnp.int32, (tokens, tokens), 1)
    )

    def column(row):
        return jnp.sum(jnp.where(eye, row, 0.0), axis=1, keepdims=True)

    factor = column(mask * scale / count[:, :tokens])
    gblk[...] = (jnp.exp(s - column(zs)) - jnp.exp(t - column(zt))) * factor
    outs = []
    mycols = pl.ds(pl.multiple_of(i * width, width), width)
    r = 1 - lax.rem(i, 2)
    for h in range(2):
        outs.append(
            remote(gblk, grad_ref.at[:, mycols], g_send.at[h], g_recv.at[lax.div(i, 2)], {"mx": 2 * h + r, "my": k})
        )
    for copy in outs:
        copy.start()

    for copy in lx:
        copy.wait_recv()
    los_y[iy] = jnp.sum(los_x[...], axis=0)
    ly = spread(los_y, iy, 1, y_send, y_recv, ypeers)

    forwards = []
    for n in range(2):
        j = 2 * n + 1 - c
        cols = pl.ds(pl.multiple_of(j * width, width), width)
        block = grad_ref.at[:, cols]
        pltpu.make_async_copy(block, block, g_recv.at[n]).wait()
        copy = remote(block, block, f_send.at[n], f_recv.at[n], {"mx": partner})
        copy.start()
        forwards.append(copy)

    for copy in ly:
        copy.wait_recv()
    loss_ref[...] = jnp.sum(los_y[...], axis=0) / count
    for copy in forwards:
        copy.wait_recv()
    for copy in swaps + first + cx + cy + sts + lx + outs + ly + forwards:
        copy.wait_send()


def finish(grad, mis, loss, grad_out, mis_out, loss_out, sem):
    copies = [
        pltpu.make_async_copy(src, dst, sem.at[n])
        for n, (src, dst) in enumerate(((grad, grad_out), (mis, mis_out), (loss, loss_out)))
    ]
    for copy in copies:
        copy.start()
    for copy in copies:
        copy.wait()


def local(xt, wt, xs, ws, mask):
    nx, ny, nk, ni = (lax.axis_size(a) for a in ("dp_0", "dp_1", "mx", "my"))
    tokens, depth_t = xt.shape
    width = wt.shape[1]
    depth_s, span = ws.shape
    scale = HEAT * width * nk * ni * tokens * nx * ny
    f32 = jnp.float32
    dma = pltpu.SemaphoreType.DMA
    vmem = pl.BlockSpec(memory_space=pltpu.VMEM)
    hbm = pl.BlockSpec(memory_space=pltpu.HBM)
    grad, mis, loss = pl.pallas_call(
        functools.partial(kernel, (nx, ny, nk, ni), scale),
        out_shape=(
            pltpu.VMEM((tokens, span), f32),
            pltpu.VMEM((1, tokens), f32),
            pltpu.VMEM((1, 128), f32),
        ),
        in_specs=[hbm] * 5,
        out_specs=(vmem, vmem, vmem),
        scratch_shapes=[
            pltpu.VMEM((tokens, depth_t), jnp.bfloat16),
            pltpu.VMEM((depth_t, width), jnp.bfloat16),
            pltpu.VMEM((tokens, depth_s), jnp.bfloat16),
            pltpu.VMEM((4, depth_s, width), jnp.bfloat16),
            pltpu.VMEM((1, tokens), jnp.int32),
            pltpu.VMEM((2, tokens, width), f32),
            pltpu.VMEM((2, tokens, width), f32),
            pltpu.VMEM((2, tokens, width), f32),
            pltpu.VMEM((2, tokens, width), f32),
            pltpu.VMEM((tokens, width), f32),
            pltpu.VMEM((nk * ni, 2, 128), f32),
            pltpu.VMEM((nx, 1, 128), f32),
            pltpu.VMEM((ny, 1, 128), f32),
            pltpu.VMEM((nx, 1, 128), f32),
            pltpu.VMEM((ny, 1, 128), f32),
            dma((7 + CHUNKS,)),
            dma((2,)),
            dma((2,)),
            dma((2,)),
            dma((2,)),
            dma((nk * ni,)),
            dma((nk * ni,)),
            dma((2,)),
            dma((2,)),
            dma((2,)),
            dma((2,)),
            dma((2, nx)),
            dma((2, nx)),
            dma((2, ny)),
            dma((2, ny)),
        ],
        compiler_params=pltpu.CompilerParams(collective_id=0, has_side_effects=True, vmem_limit_bytes=63000000),
    )(xt, wt, xs, ws, mask.reshape(1, tokens))
    grad, mis, loss = pl.pallas_call(
        finish,
        out_shape=(
            jax.ShapeDtypeStruct((tokens, span), f32),
            jax.ShapeDtypeStruct((1, tokens), f32),
            jax.ShapeDtypeStruct((1, 128), f32),
        ),
        in_specs=[vmem] * 3,
        out_specs=(hbm,) * 3,
        scratch_shapes=[dma((3,))],
        compiler_params=pltpu.CompilerParams(vmem_limit_bytes=1 << 20),
    )(grad, mis, loss)
    return mis.reshape(tokens), loss[0, 0], grad


def solution(mesh):
    split = Mesh(
        mesh.devices.reshape(4, 8, mesh.shape["mx"], mesh.shape["my"]), ("dp_0", "dp_1", "mx", "my")
    )
    in_specs = (P(DP, None), P(None, ("mx", "my")), P(DP, "mx"), P("mx", "my"), P(DP))
    out_specs = (P(DP), P(), P(DP, "my"))
    return jax.shard_map(local, mesh=split, in_specs=in_specs, out_specs=out_specs, check_vma=False)
```
